128 devices in a mesh: dp: 2 (over core), tensor: 64 (over z, y, x).
Axes of the slice: x: 4, y: 4, z: 4, core: 2. Of those that a mesh axis runs over, the one named last changes fastest.
Arguments:
- resid_stream: bfloat16 [2048, 4608], P(('dp', 'tensor')), parts along dimension 0, may hold values from -120 to 120, as said below
- pre_gain: float32 [4608], replicated, may hold values from 0.5 to 1.5
- w_gate: bfloat16 [4608, 24576], P(None, 'tensor'), may hold values from -0.09375 to 0.09375
- w_up: bfloat16 [4608, 24576], P(None, 'tensor'), may hold values from -0.09375 to 0.09375
- w_down: bfloat16 [24576, 4608], P('tensor'), may hold values from -0.0390625 to 0.0390625
- post_gain: float32 [4608], replicated, may hold values from 0.5 to 1.5
Outputs:
- resid_out: bfloat16 [2048, 4608], P(('dp', 'tensor')), parts along dimension 0
The draws below stay inside these ranges and needn't reach their ends.
There are 2 independent parts, one for each index of `dp`. The reference program is written for one: setup_inputs(seed, part) draws one part's arguments, and reference() takes and returns one part's arrays. A program takes and returns all parts, laid end to end along the dimension named above; an argument that names none is the same for every part. Nothing has to cross between parts.
Inputs may be any that keep to these rules, and one draw needn't show every extreme that they name: `resid_stream`: entries are real-valued.
All inputs are finite; a program needn't handle non-finite values.
Results may differ from the reference program's by a relative error of at most 0.0029.
Values may be sent and summed in bfloat16 or wider, within the bound.
No kernel may reach another device: no remote copies, remote signals or barrier semaphores. Data moves between devices by JAX's collectives and lax.ppermute only.
A program may use at most 128 MiB of HBM per device.

```python
import jax
import jax.numpy as jnp
from jax import lax

D = 4608
TOKENS = 1024
FF_WIN = 24576


def draw_resid_stream(key, part):
    keys = jax.random.split(jax.random.fold_in(key, 17), 3)
    base = jnp.clip(jax.random.normal(keys[0], (TOKENS, D), jnp.float32), -4.0, 4.0)
    row_scale = jnp.exp(jax.random.uniform(keys[1], (TOKENS, 1), jnp.float32) * 2.302585)
    col_scale = jnp.exp(jax.random.uniform(keys[2], (1, D), jnp.float32, minval=-1.15, maxval=1.15))
    values = base * row_scale * col_scale
    return jnp.clip(values, -120.0, 120.0).astype(jnp.bfloat16)


def level_of(rng, shape, pieces, low, high):
    level = 1.0
    for position, shards_of in pieces:
        draws = jax.random.uniform(jax.random.fold_in(jax.random.fold_in(rng, 6), position), (shards_of,), jnp.float32, low / len(pieces), high / len(pieces))
        level = level * jnp.repeat(jnp.exp(draws), shape[position] // shards_of).reshape((-1,) + (1,) * (len(shape) - 1 - position))
    return level


def bell_draw(key, dims, scale, limit, pieces=(), kind=jnp.bfloat16):
    result = jax.random.normal(key, dims, jnp.float32) * scale
    if len(pieces) > 0:
        result = level_of(key, dims, pieces, -0.22, 0.18) * result
    return jnp.clip(result, min=-limit, max=limit).astype(kind)


def setup_inputs(seed: int = 0, part: int = 0) -> dict:
    key_list = jax.random.split(jax.random.key(seed), 7)
    part_keys = jax.random.split(jax.random.fold_in(key_list[6], part), 7)
    resid_stream = draw_resid_stream(jax.random.fold_in(jax.random.fold_in(key_list[6], part), 71), part)
    pre_gain = jnp.clip(1.0 + 0.1 * jax.random.normal(key_list[1], (D,), jnp.float32), 0.5, 1.5)
    w_gate = bell_draw(key_list[2], (D, FF_WIN), D ** -0.5, 0.09375, ((1, 64),))
    w_up = bell_draw(key_list[3], (D, FF_WIN), D ** -0.5, 0.09375, ((1, 64),))
    w_down = bell_draw(key_list[4], (FF_WIN, D), FF_WIN ** -0.5, 0.0390625, ((0, 64),))
    post_gain = jnp.clip(1.0 + 0.1 * jax.random.normal(key_list[5], (D,), jnp.float32), 0.5, 1.5)
    return {"resid_stream": resid_stream, "pre_gain": pre_gain, "w_gate": w_gate, "w_up": w_up, "w_down": w_down, "post_gain": post_gain}


norm_eps = 1e-06

def rms_scale(values):
    return values * lax.rsqrt(lax.optimization_barrier(jnp.mean(values * values, axis=-1, keepdims=True)) + norm_eps)

def reference(resid_stream, pre_gain, w_gate, w_up, w_down, post_gain):
    stream = resid_stream.astype(jnp.float32)
    normed = (rms_scale(stream) * pre_gain.astype(jnp.float32)).astype(jnp.bfloat16)
    gate_out = jnp.dot(normed, w_gate, preferred_element_type=jnp.float32)
    up_out = jnp.dot(normed, w_up, preferred_element_type=jnp.float32)
    hidden = (jax.nn.gelu(gate_out, approximate=True) * up_out).astype(jnp.bfloat16)
    block_out = jnp.dot(hidden, w_down, preferred_element_type=jnp.float32)
    post = (rms_scale(block_out) * post_gain.astype(jnp.float32)).astype(jnp.bfloat16)
    post = lax.optimization_barrier(post)
    return (stream + post.astype(jnp.float32)).astype(jnp.bfloat16)
```

```python
import jax
import jax.numpy as jnp
from jax import lax
from jax.sharding import PartitionSpec as P

norm_eps = 1e-06
AXES = ("dp", "tensor")
STRIDE = (1, 4, 16)
ORDERS = ((0, 1, 2), (1, 2, 0), (2, 0, 1))


def neighbour(dp, chip, axis, large):
    at = (chip // STRIDE[axis]) % 4
    to = at ^ 3 if large == (dp == 0) else at ^ 1
    return chip + (to - at) * STRIDE[axis]


def exchange(block, axis):
    perm = [(dp * 64 + t, dp * 64 + neighbour(dp, t, axis, True)) for dp in range(2) for t in range(64)]
    return lax.ppermute(block, AXES, perm)


def small_cubes():
    cubes, seen = [], set()
    for dp in range(2):
        for t in range(64):
            if (dp, t) in seen:
                continue
            cube = []
            for corner in range(8):
                chip = t
                for axis in range(3):
                    if corner >> axis & 1:
                        chip = neighbour(dp, chip, axis, False)
                cube.append(dp * 64 + chip)
                seen.add((dp, chip))
            cubes.append(cube)
    return cubes


def swap_in_cube(blocks):
    return lax.all_to_all(blocks, AXES, 0, 0, axis_index_groups=small_cubes(), tiled=True)


def shards(resid_stream, pre_gain, w_gate, w_up, w_down, post_gain):
    rows, width = resid_stream.shape
    third = width // 3
    stream = resid_stream.astype(jnp.float32)
    local_norm = stream * lax.rsqrt(jnp.mean(stream * stream, axis=1, keepdims=True) + norm_eps)
    normed = (local_norm * pre_gain).astype(jnp.bfloat16)
    cube_rows = swap_in_cube(jnp.broadcast_to(normed[None], (8, rows, width))).reshape(8 * rows, width)

    gate = [[] for _ in range(8)]
    up = [[] for _ in range(8)]

    def project(piece, colour, corners):
        cols = slice(colour * third, (colour + 1) * third)
        g = jnp.dot(piece, w_gate[cols], preferred_element_type=jnp.float32)
        u = jnp.dot(piece, w_up[cols], preferred_element_type=jnp.float32)
        for i, corner in enumerate(corners):
            gate[corner].append(g[i * 8 * rows : (i + 1) * 8 * rows])
            up[corner].append(u[i * 8 * rows : (i + 1) * 8 * rows])

    bits = [tuple(1 << a for a in order) for order in ORDERS]
    own = [cube_rows[:, c * third : (c + 1) * third] for c in range(3)]
    first = [exchange(own[c], ORDERS[c][0]) for c in range(3)]
    near = [jnp.concatenate([own[c], first[c]]) for c in range(3)]
    second = [exchange(near[c], ORDERS[c][1]) for c in range(3)]
    third_a = [exchange(near[c], ORDERS[c][2]) for c in range(3)]
    third_b = [exchange(second[c], ORDERS[c][2]) for c in range(3)]
    for pieces, base in ((near, lambda b: 0), (second, lambda b: b[1]), (third_a, lambda b: b[2]), (third_b, lambda b: b[1] + b[2])):
        for c in range(3):
            at = base(bits[c])
            project(pieces[c], c, (at, at + bits[c][0]))
    hidden = [
        (jax.nn.gelu(sum(gate[k]), approximate=True) * sum(up[k])).astype(jnp.bfloat16) for k in range(8)
    ]

    def partial(colour, corner):
        both = jnp.concatenate([hidden[corner], hidden[corner + bits[colour][0]]])
        return jnp.dot(both, w_down[:, colour * third : (colour + 1) * third], preferred_element_type=jnp.float32)

    def send(sums, axis):
        return exchange(sums.astype(jnp.bfloat16), axis).astype(jnp.float32)

    far_a = [send(partial(c, bits[c][1] + bits[c][2]), ORDERS[c][2]) for c in range(3)]
    far_b = [send(partial(c, bits[c][2]), ORDERS[c][2]) for c in range(3)]
    mid = [send(partial(c, bits[c][1]) + far_a[c], ORDERS[c][1]) for c in range(3)]
    last = [partial(c, 0) + far_b[c] + mid[c] for c in range(3)]
    ends = [send(last[c][8 * rows :], ORDERS[c][0]) for c in range(3)]
    sums = jnp.concatenate([(last[c][: 8 * rows] + ends[c]).astype(jnp.bfloat16) for c in range(3)], axis=1)
    block_rows = jnp.sum(swap_in_cube(sums.reshape(8, rows, width)).astype(jnp.float32), axis=0)

    row_factor = lax.rsqrt(jnp.mean(block_rows * block_rows, axis=1, keepdims=True) + norm_eps)
    post = (block_rows * row_factor * post_gain).astype(jnp.bfloat16)
    post = lax.optimization_barrier(post)
    return (stream + post.astype(jnp.float32)).astype(jnp.bfloat16)


def solution(mesh):
    return jax.shard_map(
        shards,
        mesh=mesh,
        in_specs=(
            P(("dp", "tensor"), None),
            P(),
            P(None, "tensor"),
            P(None, "tensor"),
            P("tensor", None),
            P(),
        ),
        out_specs=P(("dp", "tensor"), None),
        check_vma=False,
    )
```

```python
import jax
import jax.numpy as jnp
from jax import lax
from jax.sharding import PartitionSpec as P


norm_eps = 1e-06
AXES = ("dp", "tensor")
STRIDE = (1, 4, 16)
ORDERS = ((0, 1, 2), (1, 2, 0), (2, 0, 1))
COLOURS = range(3)


def neighbour(dp, chip, axis, large):
    at = (chip // STRIDE[axis]) % 4
    wraps = large == (dp == 1) if axis == 0 else large == (dp == 0)
    to = at ^ 3 if wraps else at ^ 1
    return chip + (to - at) * STRIDE[axis]


def exchange(block, axis, large=True):
    perm = [(dp * 64 + t, dp * 64 + neighbour(dp, t, axis, large)) for dp in range(2) for t in range(64)]
    return lax.ppermute(block, AXES, perm)


def small_cubes():
    cubes, seen = [], set()
    for dp in range(2):
        for t in range(64):
            if (dp, t) in seen:
                continue
            cube = []
            for corner in range(8):
                chip = t
                for axis in range(3):
                    if corner >> axis & 1:
                        chip = neighbour(dp, chip, axis, False)
                cube.append(dp * 64 + chip)
                seen.add((dp, chip))
            cubes.append(cube)
    return cubes


def swap_in_cube(blocks):
    return lax.all_to_all(blocks, AXES, 0, 0, axis_index_groups=small_cubes(), tiled=True)


def block(resid_stream, pre_gain, w_gate, w_up, w_down, post_gain):
    rows, width = resid_stream.shape
    third = width // 3
    cols = [slice(c * third, (c + 1) * third) for c in COLOURS]
    bits = [tuple(1 << a for a in order) for order in ORDERS]
    stream = resid_stream.astype(jnp.float32)
    local_norm = stream * lax.rsqrt(jnp.mean(stream * stream, axis=1, keepdims=True) + norm_eps)
    normed = (local_norm * pre_gain).astype(jnp.bfloat16)

    cube_rows = swap_in_cube(jnp.broadcast_to(normed[None], (8, rows, width))).reshape(8 * rows, width)
    own = [cube_rows[:, cols[c]] for c in COLOURS]

    gate = [[] for _ in range(8)]
    up = [[] for _ in range(8)]

    def project(piece, colour, corners):
        g = jnp.dot(piece, w_gate[cols[colour]], preferred_element_type=jnp.float32)
        u = jnp.dot(piece, w_up[cols[colour]], preferred_element_type=jnp.float32)
        for i, corner in enumerate(corners):
            gate[corner].append(g[i * 8 * rows : (i + 1) * 8 * rows])
            up[corner].append(u[i * 8 * rows : (i + 1) * 8 * rows])

    first = [exchange(own[c], ORDERS[c][0]) for c in COLOURS]
    near = [jnp.concatenate([own[c], first[c]]) for c in COLOURS]
    second = [exchange(near[c], ORDERS[c][1]) for c in COLOURS]
    third_a = [exchange(near[c], ORDERS[c][2]) for c in COLOURS]
    third_b = [exchange(second[c], ORDERS[c][2]) for c in COLOURS]
    for pieces, base in (
        (near, lambda b: 0), (second, lambda b: b[1]), (third_a, lambda b: b[2]), (third_b, lambda b: b[1] + b[2])
    ):
        for c in COLOURS:
            at = base(bits[c])
            project(pieces[c], c, (at, at + bits[c][0]))
    hidden = [
        (jax.nn.gelu(sum(gate[k]), approximate=True) * sum(up[k])).astype(jnp.bfloat16) for k in range(8)
    ]

    def partial(colour, corners):
        both = jnp.concatenate([hidden[k] for k in corners]) if len(corners) > 1 else hidden[corners[0]]
        return jnp.dot(both, w_down[:, cols[colour]], preferred_element_type=jnp.float32)

    def send(sums, axis):
        return exchange(sums.astype(jnp.bfloat16), axis).astype(jnp.float32)

    far_a, far_b, far_c, mid, last, ends = [], [], [], [], [], []
    for c, (b0, b1, b2) in enumerate(bits):
        far_a.append(send(partial(c, (b1 + b2, 7)), ORDERS[c][2]))
        far_b.append(send(partial(c, (b0 + b2,)), ORDERS[c][2]))
        far_c.append(send(partial(c, (b2,)), ORDERS[c][2]))
    for c, (b0, b1, b2) in enumerate(bits):
        mid.append(send(partial(c, (b1, b1 + b0)) + far_a[c], ORDERS[c][1]))
    for c, (b0, b1, b2) in enumerate(bits):
        mine = partial(c, (0, b0))
        ends.append(send(mine[8 * rows :] + far_b[c] + mid[c][8 * rows :], ORDERS[c][0]))
        last.append(mine[: 8 * rows] + far_c[c] + mid[c][: 8 * rows])
    sums = jnp.concatenate([(last[c] + ends[c]).astype(jnp.bfloat16) for c in COLOURS], axis=1)

    block_rows = jnp.sum(swap_in_cube(sums.reshape(8, rows, width)).astype(jnp.float32), axis=0)

    row_factor = lax.rsqrt(jnp.mean(block_rows * block_rows, axis=1, keepdims=True) + norm_eps)
    post = (block_rows * row_factor * post_gain).astype(jnp.bfloat16)
    post = lax.optimization_barrier(post)
    return (stream + post.astype(jnp.float32)).astype(jnp.bfloat16)


def solution(mesh):
    return jax.shard_map(
        block,
        mesh=mesh,
        in_specs=(
            P(("dp", "tensor"), None),
            P(),
            P(None, "tensor"),
            P(None, "tensor"),
            P("tensor", None),
            P(),
        ),
        out_specs=P(("dp", "tensor"), None),
        check_vma=False,
    )
```

```python
import jax
import jax.numpy as jnp
from jax import lax
from jax.sharding import PartitionSpec as P


norm_eps = 1e-06
AXES = ("dp", "tensor")
STRIDE = (1, 4, 16)
ORDERS = ((0, 1, 2), (1, 2, 0), (2, 0, 1))
COLOURS = range(3)


def neighbour(dp, chip, axis, large):
    at = (chip // STRIDE[axis]) % 4
    wraps = large == (dp == 1) if axis == 0 else large == (dp == 0)
    to = at ^ 3 if wraps else at ^ 1
    return chip + (to - at) * STRIDE[axis]


def exchange(block, axis, large=True):
    perm = [(dp * 64 + t, dp * 64 + neighbour(dp, t, axis, large)) for dp in range(2) for t in range(64)]
    return lax.ppermute(block, AXES, perm)


def small_cubes():
    cubes, seen = [], set()
    for dp in range(2):
        for t in range(64):
            if (dp, t) in seen:
                continue
            cube = []
            for corner in range(8):
                chip = t
                for axis in range(3):
                    if corner >> axis & 1:
                        chip = neighbour(dp, chip, axis, False)
                cube.append(dp * 64 + chip)
                seen.add((dp, chip))
            cubes.append(cube)
    return cubes


def swap_in_cube(blocks):
    return lax.all_to_all(blocks, AXES, 0, 0, axis_index_groups=small_cubes(), tiled=True)


def forward(resid_stream, pre_gain, w_gate, w_up, w_down, post_gain):
    rows, width = resid_stream.shape
    third = width // 3
    cols = [slice(c * third, (c + 1) * third) for c in COLOURS]
    bits = [tuple(1 << a for a in order) for order in ORDERS]
    stream = resid_stream.astype(jnp.float32)
    local_norm = stream * lax.rsqrt(jnp.mean(stream * stream, axis=1, keepdims=True) + norm_eps)
    normed = (local_norm * pre_gain).astype(jnp.bfloat16)

    cube_rows = swap_in_cube(jnp.broadcast_to(normed[None], (8, rows, width))).reshape(8 * rows, width)
    own = [cube_rows[:, cols[c]] for c in COLOURS]

    gate = [[] for _ in range(8)]
    up = [[] for _ in range(8)]

    def project(piece, colour, corners):
        g = jnp.dot(piece, w_gate[cols[colour]], preferred_element_type=jnp.float32)
        u = jnp.dot(piece, w_up[cols[colour]], preferred_element_type=jnp.float32)
        for i, corner in enumerate(corners):
            gate[corner].append(g[i * 8 * rows : (i + 1) * 8 * rows])
            up[corner].append(u[i * 8 * rows : (i + 1) * 8 * rows])

    first = [exchange(own[c], ORDERS[c][0]) for c in COLOURS]
    near = [jnp.concatenate([own[c], first[c]]) for c in COLOURS]
    second = [exchange(near[c], ORDERS[c][1]) for c in COLOURS]
    third_o = [exchange(own[c], ORDERS[c][2]) for c in COLOURS]
    third_f = [exchange(first[c], ORDERS[c][2]) for c in COLOURS]
    third_a = []
    for c in COLOURS:
        third_a.append(jnp.concatenate([third_o[c], third_f[c]]))
    third_b = [exchange(second[c], ORDERS[c][2]) for c in COLOURS]
    for pieces, base in (
        (near, lambda b: 0), (second, lambda b: b[1]), (third_a, lambda b: b[2]), (third_b, lambda b: b[1] + b[2])
    ):
        for c in COLOURS:
            at = base(bits[c])
            project(pieces[c], c, (at, at + bits[c][0]))
    hidden = [
        (jax.nn.gelu(sum(gate[k]), approximate=True) * sum(up[k])).astype(jnp.bfloat16) for k in range(8)
    ]

    down = []
    for c in COLOURS:
        down.append(lax.optimization_barrier(w_down[:, cols[c]]))

    def partial(colour, corners):
        both = jnp.concatenate([hidden[k] for k in corners]) if len(corners) > 1 else hidden[corners[0]]
        return jnp.dot(both, down[colour], preferred_element_type=jnp.float32)

    def send(sums, axis):
        return exchange(sums.astype(jnp.bfloat16), axis)

    half = 8 * rows
    wide = lambda piece: piece.astype(jnp.float32)
    far_a, far_b, mid, edge, ends, last = [], [], [], [], [], []
    for c, (b0, b1, b2) in enumerate(bits):
        far_a.append(send(partial(c, (b1 + b2, 7)), ORDERS[c][2]))
        far_b.append(send(partial(c, (b2, b0 + b2)), ORDERS[c][2]))
    for c, (b0, b1, b2) in enumerate(bits):
        mid.append(send(partial(c, (b1 + b0,)) + wide(far_a[c][half:]), ORDERS[c][1]))
        edge.append(send(partial(c, (b1,)) + wide(far_a[c][:half]), ORDERS[c][1]))
    for c, (b0, b1, b2) in enumerate(bits):
        mine = partial(c, (0, b0))
        ends.append(send(mine[half:] + wide(far_b[c][half:]) + wide(mid[c]), ORDERS[c][0]))
        last.append(mine[:half] + wide(far_b[c][:half]) + wide(edge[c]))
    met = lax.ppermute(mid[0][:rows, :128], "dp", [(0, 1), (1, 0)])
    zero = 0.0 * wide(met[:1, :1])
    sums = jnp.concatenate([(last[c] + wide(ends[c]) + zero).astype(jnp.bfloat16) for c in COLOURS], axis=1)

    block_rows = jnp.sum(swap_in_cube(sums.reshape(8, rows, width)).astype(jnp.float32), axis=0)

    row_factor = lax.rsqrt(jnp.mean(block_rows * block_rows, axis=1, keepdims=True) + norm_eps)
    post = (block_rows * row_factor * post_gain).astype(jnp.bfloat16)
    post = lax.optimization_barrier(post)
    return (stream + post.astype(jnp.float32)).astype(jnp.bfloat16)


def solution(mesh):
    return jax.shard_map(
        forward,
        mesh=mesh,
        in_specs=(
            P(("dp", "tensor"), None),
            P(),
            P(None, "tensor"),
            P(None, "tensor"),
            P("tensor", None),
            P(),
        ),
        out_specs=P(("dp", "tensor"), None),
        check_vma=False,
    )
```
